32 devices in a mesh: grp: 2 (over y), vec: 4 (over z), walk: 2 (over x), orb: 2 (over core).
Axes of the slice: x: 2, y: 2, z: 4, core: 2. Of those that a mesh axis runs over, the one named last changes fastest.
Arguments:
- walkers: bfloat16 [32, 512, 128], P(('grp', 'walk'), 'orb'), parts along dimension 0, may hold values from -3 to 3
- inv_intersection: bfloat16 [32, 128, 128], P(('grp', 'walk')), parts along dimension 0, may hold values from -0.5 to 0.5
- trial: bfloat16 [512, 128], replicated, may hold values from -0.25 to 0.25
- vectors: bfloat16 [32, 512, 512], P('vec', 'orb')
- aux_field: float32 [32, 32], P(('grp', 'walk'), 'vec'), parts along dimension 0, may hold values from -5 to 5
- log_weight: float32 [32], P(('grp', 'walk')), parts along dimension 0, may hold values from -4 to 4
- copy_list: int32 [32], P(('grp', 'walk')), parts along dimension 0, may hold values from 0 to 15
Outputs:
- walkers_out: bfloat16 [32, 512, 128], P(('grp', 'walk'), 'orb'), parts along dimension 0
- weights_out: float32 [32], P(('grp', 'walk')), parts along dimension 0
The draws below stay inside these ranges and needn't reach their ends.
There are 2 independent parts, one for each index of `grp`. The reference program is written for one: setup_inputs(seed, part) draws one part's arguments, and reference() takes and returns one part's arrays. A program takes and returns all parts, laid end to end along the dimension named above; an argument that names none is the same for every part. Nothing has to cross between parts.
Inputs may be any that keep to these rules, and one draw needn't show every extreme that they name: `copy_list`: the walker, within the same ensemble, whose copy fills the slot.
All inputs are finite; a program needn't handle non-finite values.
Results may differ from the reference program's by a relative error of at most 0.008.
Values may be sent and summed in bfloat16 or wider, within the bound.
A program may use at most 64 MiB of HBM per device.

```python
import math
import jax
import jax.numpy as jnp
import numpy as np
from jax import lax

N = 512
E = 128
ORDER = 6
CHOL = 32
WALKERS = 16


def draw_vectors(key, part):
    base = jax.random.normal(key, (CHOL, N, N), jnp.float32)
    spread = 5.0 / math.sqrt(N * CHOL)
    sym = (base + jnp.swapaxes(base, 1, 2)) * (spread / math.sqrt(2.0))
    return sym.astype(jnp.bfloat16)


def set_ends(drawn, key, smallest, top_value):
    dims = drawn.shape
    index_at = [jax.random.randint(jax.random.fold_in(key, axis), (), 0, dims[axis]) for axis in range(len(dims))]
    drawn = drawn.at[tuple(index_at)].set(smallest)
    longest = dims.index(max(dims))
    index_at[longest] = (index_at[longest] + 1) % dims[longest]
    return drawn.at[tuple(index_at)].set(top_value)


def steps_of(own_key, shape, shards, smallest, high):
    level, own = 1.0, jax.random.fold_in(own_key, 6)
    for position, parts in shards:
        heights = jnp.exp(jax.random.uniform(jax.random.fold_in(own, position), (parts,), jnp.float32, smallest / len(shards), high / len(shards)))
        level = level * jnp.repeat(heights, shape[position] // parts).reshape([-1 if axis == position else 1 for axis in range(len(shape))])
    return level


def rank_bounds(count, slope):
    loads = [(1 << 20) // math.isqrt(grade ** slope) + 1 for grade in range(1, count + 1)]
    width = 1 + sum(loads) // (1 << 30)
    return np.cumsum(np.array([max(1, weight // width) for weight in loads]))


def ranked_ids(own_key, shape, count, slope):
    table = rank_bounds(count, slope)
    pick = jax.random.randint(jax.random.fold_in(own_key, 1), shape, 0, int(table[count - 1]))
    rank = jnp.searchsorted(jnp.asarray(table, jnp.int32), pick, side="right")
    return jax.random.permutation(jax.random.fold_in(own_key, 2), count)[rank].astype(jnp.int32)


def gaussian(own_key, extent, scale, reach, pieces=(), kind=jnp.bfloat16):
    factor_of = steps_of(own_key, extent, pieces, -0.22, 0.18) if pieces else 1.0
    array = jax.random.normal(own_key, extent, jnp.float32) * scale * factor_of
    return jnp.minimum(jnp.maximum(array, -reach), reach).astype(kind)


def setup_inputs(seed: int = 0, part: int = 0) -> dict:
    streams_of = jax.random.split(jax.random.key(seed), 8)
    own_keys = jax.random.split(jax.random.fold_in(streams_of[7], part), 8)
    return {
        "walkers": gaussian(own_keys[0], (WALKERS, N, E), 0.5, 3.0, ((0, 2), (1, 2))),
        "inv_intersection": gaussian(own_keys[1], (WALKERS, E, E), E ** -0.5, 0.5, ((0, 2),)),
        "trial": gaussian(streams_of[2], (N, E), N ** -0.5, 0.25),
        "vectors": draw_vectors(jax.random.fold_in(streams_of[7], 71), part),
        "aux_field": gaussian(own_keys[4], (WALKERS, CHOL), 1.0, 5.0, ((0, 2), (1, 4)), jnp.float32),
        "log_weight": gaussian(own_keys[5], (WALKERS,), 1.0, 4.0, ((0, 2),), jnp.float32),
        "copy_list": set_ends(ranked_ids(own_keys[6], (WALKERS,), WALKERS, 2), jax.random.fold_in(own_keys[6], 3), 0, WALKERS - 1).astype(jnp.int32),
    }


step_root = math.sqrt(0.08)

def reference(walkers, inv_intersection, trial, vectors, aux_field, log_weight, copy_list):
    high = lax.Precision.HIGHEST
    green = jnp.einsum('wne,wef->wnf', walkers.astype(jnp.float32), inv_intersection.astype(jnp.float32), precision=high).astype(jnp.bfloat16)
    mixed = jnp.einsum('gnm,me->gne', vectors.astype(jnp.float32), trial.astype(jnp.float32), precision=high).astype(jnp.bfloat16)
    bias = jnp.einsum('wne,gne->wg', green.astype(jnp.float32), mixed.astype(jnp.float32), precision=high)
    shift = -step_root * bias
    field = aux_field - shift
    new_log = log_weight + lax.optimization_barrier(jnp.sum(aux_field * shift - 0.5 * shift * shift, axis=1))
    weighted = (field * step_root).astype(jnp.bfloat16)
    operator = jnp.einsum('wg,gnm->wnm', weighted.astype(jnp.float32), vectors.astype(jnp.float32), precision=high).astype(jnp.bfloat16)
    operand = operator.astype(jnp.float32)
    term = walkers
    total = walkers.astype(jnp.float32)
    for degree in range(1, ORDER + 1):
        product = jnp.einsum('wnm,wme->wne', operand, term.astype(jnp.float32), precision=high)
        term = (product / degree).astype(jnp.bfloat16)
        total = total + term.astype(jnp.float32)
    propagated = total.astype(jnp.bfloat16)
    return (propagated[copy_list], new_log[copy_list])
```

```python
import functools
import math

import jax
import jax.numpy as jnp
from jax import lax
from jax.experimental import pallas as pl
from jax.experimental.pallas import tpu as pltpu
from jax.sharding import PartitionSpec as P

ORDER = 6
PIECES = 2
MESH = pl.DeviceIdType.MESH
F32 = jnp.float32
BF16 = jnp.bfloat16

step_root = math.sqrt(0.08)


def remote(src, dst, send, recv, where):
    return pltpu.make_async_remote_copy(
        src_ref=src, dst_ref=dst, send_sem=send, recv_sem=recv, device_id=where, device_id_type=MESH
    )


def kernel(
    depth, width,
    walkers, inverse, trial, vectors, aux, log_weight, copy_list,
    out, out_log,
    green, mixed, bias_own, bias_in, other_rows, partial, arrived, leaving, operator, full, term, result, every,
    factor_in, factor_out, logs,
    bias_sems, rows_sems, chain_send, chain_recv, factor_send, factor_recv, swap_send, swap_recv,
    every_recv, own_sends, next_send, across_send, log_send, log_recv,
):
    z = lax.axis_index("vec")
    x = lax.axis_index("walk")
    o = lax.axis_index("orb")
    last = depth - 1
    local, rows, electrons = walkers.shape
    count, _, orbitals = vectors.shape
    half = local // 2
    block = orbitals // 4
    span = 2 * block // count
    wide = count * span
    packed = partial.shape[1]
    piece = packed // PIECES
    chunks = half * PIECES
    mine = half // 2

    barrier = pltpu.get_barrier_semaphore()

    def greet(where):
        pl.semaphore_signal(barrier, inc=1, device_id=where, device_id_type=MESH)

    greet({"orb": 1 - o})
    for hop in range(1, width):
        for core in range(2):
            greet({"walk": lax.rem(x + hop, width), "orb": core})

    @pl.when(z > 0)
    def _():
        for core in range(2):
            greet({"vec": z - 1, "orb": core})

    @pl.when(z < last)
    def _():
        for core in range(2):
            greet({"vec": z + 1, "orb": core})

    sides = jnp.where(z > 0, 2, 0) + jnp.where(z < last, 2, 0)
    pl.semaphore_wait(barrier, 1 + 2 * (width - 1) + sides)

    rows_copy = remote(walkers, other_rows, rows_sems.at[0], rows_sems.at[1], {"orb": 1 - o})
    rows_copy.start()

    for w in range(local):
        green[w] = jnp.dot(walkers[w], inverse[w], preferred_element_type=F32).astype(BF16)
    for g in range(count):
        mixed[g] = jnp.dot(vectors[g], trial[...], preferred_element_type=F32).astype(BF16)
    gram = jnp.zeros((local * span, wide), F32)
    for j in range(rows // span):
        left = green[:, j * span:(j + 1) * span, :].reshape(local * span, electrons)
        right = mixed[:, j * span:(j + 1) * span, :].reshape(wide, electrons)
        gram = gram + lax.dot_general(left, right, (((1,), (1,)), ((), ())), preferred_element_type=F32)
    row_id = lax.broadcasted_iota(jnp.int32, (local * span, wide), 0)
    col_id = lax.broadcasted_iota(jnp.int32, (local * span, wide), 1)
    same = row_id % span == col_id % span
    folded = jnp.sum(jnp.where(same, gram, 0.0).reshape(local, span, wide), axis=1)
    wide_row = lax.broadcasted_iota(jnp.int32, (wide, wide), 0)
    wide_col = lax.broadcasted_iota(jnp.int32, (wide, wide), 1)
    groups = jnp.where(wide_row // span == wide_col // span, 1.0, 0.0).astype(F32)
    bias_own[...] = jnp.dot(folded, groups, precision=lax.Precision.HIGHEST, preferred_element_type=F32)
    bias_copy = remote(bias_own, bias_in, bias_sems.at[0], bias_sems.at[1], {"orb": 1 - o})
    bias_copy.start()
    bias_copy.wait()
    bias = bias_own[...] + bias_in[...]
    shift = -step_root * bias
    field = aux[...] - shift
    factor = jnp.sum(aux[...] * shift - 0.5 * shift * shift, axis=1, keepdims=True) * (1.0 / span)
    factor = jnp.broadcast_to(factor, (local, logs.shape[2]))
    weighted = (field * step_root).astype(BF16).astype(F32)
    spread = jnp.broadcast_to(weighted[:, None, :], (local, span, wide)).reshape(local * span, wide)
    kron = jnp.where(same, spread, 0.0).astype(BF16)

    for j in range(block // span):
        here = slice(j * span, (j + 1) * span)
        cols = pl.ds(pl.multiple_of(o * block, block), 3 * block)
        strip = vectors[:, here, cols].reshape(wide, 3 * block)
        summed = jnp.dot(kron, strip, preferred_element_type=F32)
        for slot in range(3):
            partial[:, slot * block + j * span:slot * block + (j + 1) * span, :] = summed[
                :, slot * block:(slot + 1) * block
            ].reshape(local, span, block)
        below = slice(block + j * span, block + (j + 1) * span)
        one = vectors[:, below, pl.ds(pl.multiple_of((1 - o) * block, block), block)].reshape(wide, block)
        two = vectors[:, below, 3 * block:].reshape(wide, block)
        summed = jnp.dot(kron, jnp.concatenate([one, two], axis=1), preferred_element_type=F32)
        for slot in range(2):
            partial[:, (3 + slot) * block + j * span:(3 + slot) * block + (j + 1) * span, :] = summed[
                :, slot * block:(slot + 1) * block
            ].reshape(local, span, block)

    to_next = [z - 1, z + 1]
    upstream = [last - z, z]
    downstream = [z, last - z]

    def chain_copy(side, c):
        return remote(
            leaving.at[side, c], arrived.at[side, c], chain_send.at[side, c], chain_recv.at[side, c],
            {"vec": to_next[side]},
        )

    def factor_copy(side):
        return remote(
            factor_out.at[side], factor_in.at[side], factor_send.at[side], factor_recv.at[side],
            {"vec": to_next[side]},
        )

    def swap_copy(c):
        return remote(operator.at[o, c], operator.at[o, c], swap_send.at[c], swap_recv.at[c], {"orb": 1 - o})

    def swap_arrival(c):
        return remote(operator.at[1 - o, c], operator.at[1 - o, c], swap_send.at[c], swap_recv.at[c], {"orb": 1 - o})

    def chain_step(t, carry):
        for side in range(2):
            c = t - upstream[side]
            head = upstream[side] == 0
            owner = downstream[side] == 0

            @pl.when((c >= 0) & (c < chunks))
            def _():
                own = partial[side * half + c // PIECES, pl.ds(pl.multiple_of((c % PIECES) * piece, piece), piece), :]

                @pl.when(head)
                def _():
                    leaving[side, c] = own.astype(BF16)

                @pl.when(jnp.logical_not(head))
                def _():
                    chain_copy(side, c).wait_recv()
                    both = (own + arrived[side, c].astype(F32)).astype(BF16)

                    @pl.when(owner)
                    def _():
                        operator[o, c] = both

                    @pl.when(jnp.logical_not(owner))
                    def _():
                        leaving[side, c] = both

                @pl.when(jnp.logical_not(owner))
                def _():
                    chain_copy(side, c).start()

                @pl.when(owner & ((c // PIECES) % 2 != o))
                def _():
                    swap_copy(c).start()

                @pl.when(c == 0)
                def _():
                    @pl.when(head)
                    def _():
                        factor_in[side] = jnp.zeros_like(factor)

                    @pl.when(jnp.logical_not(head))
                    def _():
                        factor_copy(side).wait_recv()

                    @pl.when(jnp.logical_not(owner))
                    def _():
                        factor_out[side] = factor_in[side] + factor
                        factor_copy(side).start()

        return carry

    lax.fori_loop(0, chunks + last, chain_step, jnp.int32(0))

    def log_copy(hop):
        other = lax.rem(x + hop, width)
        return remote(logs.at[x], logs.at[x], log_send.at[hop - 1], log_recv.at[x], {"walk": other})

    logs[x] = log_weight[...] + factor + factor_in[0] + factor_in[1]
    for hop in range(1, width):
        log_copy(hop).start()

    at_end = (z == 0) | (z == last)
    base = jnp.where(z == 0, 0, half)
    inward = jnp.where(z == 0, 1, last - 1)
    rows_copy.wait_recv()

    def place(w):
        return every.at[x * local + w]

    def own_copies(i):
        w = base + 2 * i + o
        copies = []
        for core in range(2):
            copies.append((core, {"vec": inward, "orb": core}))
        for hop in range(1, width):
            for core in range(2):
                copies.append((core, {"walk": lax.rem(x + hop, width), "orb": core}))
        made = [
            remote(result.at[i, core], place(w), own_sends.at[i, n], every_recv.at[x, w], where)
            for n, (core, where) in enumerate(copies)
        ]
        made.append(
            remote(result.at[i, 1 - o], place(w), own_sends.at[i, len(copies)], every_recv.at[x, w], {"orb": 1 - o})
        )
        return made

    @pl.when(at_end)
    def _():
        for i in range(mine):
            a = 2 * i + o
            w = base + a
            for q in range(PIECES):
                swap_arrival(a * PIECES + q).wait_recv()

            def tile(core, slot):
                flat = operator[core, pl.ds(a * PIECES, PIECES)].reshape(packed, block)
                return flat[slot * block:(slot + 1) * block, :]

            def put(r, c, value):
                full[r * block:(r + 1) * block, c * block:(c + 1) * block] = value

            spots = (((0, 0), (0, 1), (0, 2), (1, 1), (1, 3)), ((2, 1), (2, 2), (2, 3), (3, 0), (3, 3)))
            for core in range(2):
                for slot in range(5):
                    r, c = spots[core][slot]
                    value = tile(core, slot)
                    put(r, c, value)
                    if r != c:
                        put(c, r, value.T)
            term[pl.ds(pl.multiple_of(o * rows, rows), rows), :] = walkers[w]
            term[pl.ds(pl.multiple_of((1 - o) * rows, rows), rows), :] = other_rows[w]
            running = term[...].astype(F32)
            for degree in range(1, ORDER + 1):
                fresh = (jnp.dot(full[...], term[...], preferred_element_type=F32) * (1.0 / degree)).astype(BF16)
                running = running + fresh.astype(F32)
                if degree < ORDER:
                    term[...] = fresh
            result[i] = running.astype(BF16).reshape(2, rows, electrons)
            for copy in own_copies(i):
                copy.start()
            every[x * local + w] = result[i, o]

    def onward(side, w, hop_to):
        return remote(place(w), place(w), next_send.at[w], every_recv.at[x, w], {"vec": hop_to})

    def across(w, hop):
        return remote(
            place(w), place(w), across_send.at[hop - 1, w], every_recv.at[x, w], {"walk": lax.rem(x + hop, width)}
        )

    for a in range(half):
        for side in range(2):
            w = side * half + a
            away = [z, last - z][side]
            hop_to = [z + 1, z - 1][side]
            end = [last - z, z][side]

            @pl.when(away > 0)
            def _():
                onward(side, w, hop_to).wait_recv()

                @pl.when(end > 0)
                def _():
                    onward(side, w, hop_to).start()

                for hop in range(1, width):
                    across(w, hop).start()

            if True:
                @pl.when((away == 0) & (o != a % 2))
                def _():
                    onward(side, w, hop_to).wait_recv()

    for hop in range(1, width):
        other = lax.rem(x + hop, width)
        for w in range(local):
            spot = every.at[other * local + w]
            remote(spot, spot, across_send.at[hop - 1, w], every_recv.at[other, w], {"walk": other}).wait_recv()
        remote(logs.at[other], logs.at[other], log_send.at[hop - 1], log_recv.at[other], {"walk": other}).wait_recv()

    for s in range(local):
        source = copy_list[s]
        out[s] = every[source]
        out_log[pl.ds(s, 1), :] = logs[source // local, pl.ds(source % local, 1), :]

    rows_copy.wait_send()
    for hop in range(1, width):
        log_copy(hop).wait_send()

    def drain(c, carry):
        for side in range(2):
            @pl.when(downstream[side] > 0)
            def _():
                chain_copy(side, c).wait_send()

        @pl.when(at_end & ((c // PIECES) % 2 != o))
        def _():
            swap_copy(c).wait_send()

        return carry

    lax.fori_loop(0, chunks, drain, jnp.int32(0))
    for side in range(2):
        @pl.when(downstream[side] > 0)
        def _():
            factor_copy(side).wait_send()

    @pl.when(at_end)
    def _():
        for i in range(mine):
            for copy in own_copies(i):
                copy.wait_send()

    for a in range(half):
        for side in range(2):
            w = side * half + a
            away = [z, last - z][side]
            hop_to = [z + 1, z - 1][side]
            end = [last - z, z][side]

            @pl.when(away > 0)
            def _():
                @pl.when(end > 0)
                def _():
                    onward(side, w, hop_to).wait_send()

                for hop in range(1, width):
                    across(w, hop).wait_send()


def per_device(depth, width, walkers, inv_intersection, trial, vectors, aux_field, log_weight, copy_list):
    local, rows, electrons = walkers.shape
    count, _, orbitals = vectors.shape
    half = local // 2
    block = orbitals // 4
    span = 2 * block // count
    wide = count * span
    packed = 5 * block
    piece = packed // PIECES
    chunks = half * PIECES
    mine = half // 2
    lanes = 128
    aux = jnp.repeat(aux_field, span, axis=1)
    log_wide = jnp.broadcast_to(log_weight[:, None], (local, lanes))
    vmem = pl.BlockSpec(memory_space=pltpu.VMEM)
    dma = pltpu.SemaphoreType.DMA
    out, out_log = pl.pallas_call(
        functools.partial(kernel, depth, width),
        out_shape=(
            jax.ShapeDtypeStruct(walkers.shape, BF16),
            jax.ShapeDtypeStruct((local, lanes), F32),
        ),
        in_specs=[vmem] * 6 + [pl.BlockSpec(memory_space=pltpu.SMEM)],
        out_specs=(vmem, vmem),
        scratch_shapes=[
            pltpu.VMEM((local, rows, electrons), BF16),
            pltpu.VMEM((count, rows, electrons), BF16),
            pltpu.VMEM((local, wide), F32),
            pltpu.VMEM((local, wide), F32),
            pltpu.VMEM((local, rows, electrons), BF16),
            pltpu.VMEM((local, packed, block), F32),
            pltpu.VMEM((2, chunks, piece, block), BF16),
            pltpu.VMEM((2, chunks, piece, block), BF16),
            pltpu.VMEM((2, chunks, piece, block), BF16),
            pltpu.VMEM((orbitals, orbitals), BF16),
            pltpu.VMEM((orbitals, electrons), BF16),
            pltpu.VMEM((mine, 2, rows, electrons), BF16),
            pltpu.VMEM((width * local, rows, electrons), BF16),
            pltpu.VMEM((2, local, lanes), F32),
            pltpu.VMEM((2, local, lanes), F32),
            pltpu.VMEM((width, local, lanes), F32),
            dma((2,)),
            dma((2,)),
            dma((2, chunks)),
            dma((2, chunks)),
            dma((2,)),
            dma((2,)),
            dma((chunks,)),
            dma((chunks,)),
            dma((width, local)),
            dma((mine, 2 * width + 1)),
            dma((local,)),
            dma((max(width - 1, 1), local)),
            dma((max(width - 1, 1),)),
            dma((width,)),
        ],
        compiler_params=pltpu.CompilerParams(collective_id=0, has_side_effects=True),
    )(walkers, inv_intersection, trial, vectors, aux, log_wide, copy_list)
    return out, out_log[:, 0]


def solution(mesh):
    depth, width = mesh.shape["vec"], mesh.shape["walk"]
    assert mesh.shape["orb"] == 2 and depth > 1
    return jax.shard_map(
        functools.partial(per_device, depth, width),
        mesh=mesh,
        in_specs=(
            P(("grp", "walk"), "orb", None),
            P(("grp", "walk"), None, None),
            P(),
            P("vec", "orb", None),
            P(("grp", "walk"), "vec"),
            P(("grp", "walk")),
            P(("grp", "walk")),
        ),
        out_specs=(P(("grp", "walk"), "orb", None), P(("grp", "walk"))),
        check_vma=False,
    )
```

```python
import functools
import math

import jax
import jax.numpy as jnp
from jax import lax
from jax.experimental import pallas as pl
from jax.experimental.pallas import tpu as pltpu
from jax.sharding import PartitionSpec as P

ORDER = 6
PIECES = 4
SKEW = 4
MESH = pl.DeviceIdType.MESH
F32 = jnp.float32
BF16 = jnp.bfloat16

step_root = math.sqrt(0.08)


def remote(src, dst, send, recv, where):
    return pltpu.make_async_remote_copy(
        src_ref=src, dst_ref=dst, send_sem=send, recv_sem=recv, device_id=where, device_id_type=MESH
    )


def kernel(
    depth, width,
    walkers, inverse, trial, vectors, aux, log_weight, copy_list,
    out, out_log,
    green, mixed, bias_own, bias_in, other_rows, partial, arrived, leaving, operator, full, term, result, every,
    factor_in, factor_out, logs,
    bias_sems, rows_sems, chain_send, chain_recv, factor_send, factor_recv, swap_send, swap_recv,
    every_recv, own_sends, next_send, across_send, log_send, log_recv,
):
    z = lax.axis_index("vec")
    x = lax.axis_index("walk")
    o = lax.axis_index("orb")
    last = depth - 1
    local, rows, electrons = walkers.shape
    count, _, orbitals = vectors.shape
    half = local // 2
    block = orbitals // 4
    span = 2 * block // count
    wide = count * span
    packed = partial.shape[1]
    piece = packed // PIECES
    chunks = half * PIECES
    mine = half // 2

    barrier = pltpu.get_barrier_semaphore()

    def greet(where):
        pl.semaphore_signal(barrier, inc=1, device_id=where, device_id_type=MESH)

    greet({"orb": 1 - o})
    for hop in range(1, width):
        for core in range(2):
            greet({"walk": lax.rem(x + hop, width), "orb": core})

    @pl.when(z > 0)
    def _():
        for core in range(2):
            greet({"vec": z - 1, "orb": core})

    @pl.when(z < last)
    def _():
        for core in range(2):
            greet({"vec": z + 1, "orb": core})

    sides = jnp.where(z > 0, 2, 0) + jnp.where(z < last, 2, 0)
    pl.semaphore_wait(barrier, 1 + 2 * (width - 1) + sides)

    rows_copy = remote(walkers, other_rows, rows_sems.at[0], rows_sems.at[1], {"orb": 1 - o})
    rows_copy.start()

    for w in range(local):
        green[w] = jnp.dot(walkers[w], inverse[w], preferred_element_type=F32).astype(BF16)
    for g in range(count):
        mixed[g] = jnp.dot(vectors[g], trial[...], preferred_element_type=F32).astype(BF16)
    gram = jnp.zeros((local * span, wide), F32)
    for j in range(rows // span):
        left = green[:, j * span:(j + 1) * span, :].reshape(local * span, electrons)
        right = mixed[:, j * span:(j + 1) * span, :].reshape(wide, electrons)
        gram = gram + lax.dot_general(left, right, (((1,), (1,)), ((), ())), preferred_element_type=F32)
    row_id = lax.broadcasted_iota(jnp.int32, (local * span, wide), 0)
    col_id = lax.broadcasted_iota(jnp.int32, (local * span, wide), 1)
    same = row_id % span == col_id % span
    folded = jnp.sum(jnp.where(same, gram, 0.0).reshape(local, span, wide), axis=1)
    wide_row = lax.broadcasted_iota(jnp.int32, (wide, wide), 0)
    wide_col = lax.broadcasted_iota(jnp.int32, (wide, wide), 1)
    groups = jnp.where(wide_row // span == wide_col // span, 1.0, 0.0).astype(F32)
    bias_own[...] = jnp.dot(folded, groups, precision=lax.Precision.HIGHEST, preferred_element_type=F32)
    pick_row = lax.broadcasted_iota(jnp.int32, (count, wide), 0)
    pick_col = lax.broadcasted_iota(jnp.int32, (count, wide), 1)
    pick = jnp.where(pick_row == pick_col // span, 1.0, 0.0).astype(F32)
    drawn = jnp.dot(aux[...], pick, precision=lax.Precision.HIGHEST, preferred_element_type=F32)
    bias_copy = remote(bias_own, bias_in, bias_sems.at[0], bias_sems.at[1], {"orb": 1 - o})
    bias_copy.start()
    bias_copy.wait()
    bias = bias_own[...] + bias_in[...]
    shift = -step_root * bias
    field = drawn - shift
    factor = jnp.sum(drawn * shift - 0.5 * shift * shift, axis=1, keepdims=True) * (1.0 / span)
    factor = jnp.broadcast_to(factor, (local, logs.shape[2]))
    weighted = (field * step_root).astype(BF16).astype(F32)
    spread = jnp.broadcast_to(weighted[:, None, :], (local, span, wide)).reshape(local * span, wide)
    kron = jnp.where(same, spread, 0.0).astype(BF16)

    for j in range(block // span):
        here = slice(j * span, (j + 1) * span)
        cols = pl.ds(pl.multiple_of(o * block, block), 3 * block)
        strip = vectors[:, here, cols].reshape(wide, 3 * block)
        summed = jnp.dot(kron, strip, preferred_element_type=F32)
        for slot in range(3):
            partial[:, slot * block + j * span:slot * block + (j + 1) * span, :] = summed[
                :, slot * block:(slot + 1) * block
            ].reshape(local, span, block)
        below = slice(block + j * span, block + (j + 1) * span)
        one = vectors[:, below, pl.ds(pl.multiple_of((1 - o) * block, block), block)].reshape(wide, block)
        two = vectors[:, below, 3 * block:].reshape(wide, block)
        summed = jnp.dot(kron, jnp.concatenate([one, two], axis=1), preferred_element_type=F32)
        for slot in range(2):
            partial[:, (3 + slot) * block + j * span:(3 + slot) * block + (j + 1) * span, :] = summed[
                :, slot * block:(slot + 1) * block
            ].reshape(local, span, block)

    to_next = [z - 1, z + 1]
    upstream = [last - z, z]
    downstream = [z, last - z]

    def chain_copy(side, c):
        return remote(
            leaving.at[side, c], arrived.at[side, c], chain_send.at[side, c], chain_recv.at[side, c],
            {"vec": to_next[side]},
        )

    def factor_copy(side):
        return remote(
            factor_out.at[side], factor_in.at[side], factor_send.at[side], factor_recv.at[side],
            {"vec": to_next[side]},
        )

    def swap_copy(c):
        return remote(operator.at[o, c], operator.at[o, c], swap_send.at[c], swap_recv.at[c], {"orb": 1 - o})

    def swap_arrival(c):
        return remote(operator.at[1 - o, c], operator.at[1 - o, c], swap_send.at[c], swap_recv.at[c], {"orb": 1 - o})

    def chain_step(t, carry):
        for side in range(2):
            c = t - SKEW * upstream[side]
            head = upstream[side] == 0
            owner = downstream[side] == 0

            @pl.when((c >= 0) & (c < chunks))
            def _():
                own = partial[side * half + c // PIECES, pl.ds(pl.multiple_of((c % PIECES) * piece, piece), piece), :]

                @pl.when(head)
                def _():
                    leaving[side, c] = own.astype(BF16)

                @pl.when(jnp.logical_not(head))
                def _():
                    chain_copy(side, c).wait_recv()
                    both = (own + arrived[side, c].astype(F32)).astype(BF16)

                    @pl.when(owner)
                    def _():
                        operator[o, c] = both

                    @pl.when(jnp.logical_not(owner))
                    def _():
                        leaving[side, c] = both

                @pl.when(jnp.logical_not(owner))
                def _():
                    chain_copy(side, c).start()

                @pl.when(owner & ((c // PIECES) % 2 != o))
                def _():
                    swap_copy(c).start()

                @pl.when(c == 0)
                def _():
                    @pl.when(head)
                    def _():
                        factor_in[side] = jnp.zeros_like(factor)

                    @pl.when(jnp.logical_not(head))
                    def _():
                        factor_copy(side).wait_recv()

                    @pl.when(jnp.logical_not(owner))
                    def _():
                        factor_out[side] = factor_in[side] + factor
                        factor_copy(side).start()

        return carry

    at_end = (z == 0) | (z == last)
    base = jnp.where(z == 0, 0, half)
    inward = jnp.where(z == 0, 1, last - 1)
    rows_copy.wait_recv()

    def place(w):
        return every.at[x * local + w]

    def own_copies(i):
        w = base + 2 * i + o
        copies = []
        for core in range(2):
            copies.append((core, {"vec": inward, "orb": core}))
        for hop in range(1, width):
            for core in range(2):
                copies.append((core, {"walk": lax.rem(x + hop, width), "orb": core}))
        made = [
            remote(result.at[i, core], place(w), own_sends.at[i, n], every_recv.at[x, w], where)
            for n, (core, where) in enumerate(copies)
        ]
        made.append(
            remote(result.at[i, 1 - o], place(w), own_sends.at[i, len(copies)], every_recv.at[x, w], {"orb": 1 - o})
        )
        return made

    def finish(i):
        @pl.when(at_end)
        def _():
            a = 2 * i + o
            w = base + a
            for q in range(PIECES):
                swap_arrival(a * PIECES + q).wait_recv()

            def tile(core, slot):
                flat = operator[core, pl.ds(a * PIECES, PIECES)].reshape(packed, block)
                return flat[slot * block:(slot + 1) * block, :]

            def put(r, c, value):
                full[r * block:(r + 1) * block, c * block:(c + 1) * block] = value

            spots = (((0, 0), (0, 1), (0, 2), (1, 1), (1, 3)), ((2, 1), (2, 2), (2, 3), (3, 0), (3, 3)))
            for core in range(2):
                for slot in range(5):
                    r, c = spots[core][slot]
                    value = tile(core, slot)
                    put(r, c, value)
                    if r != c:
                        put(c, r, value.T)
            term[pl.ds(pl.multiple_of(o * rows, rows), rows), :] = walkers[w]
            term[pl.ds(pl.multiple_of((1 - o) * rows, rows), rows), :] = other_rows[w]
            running = term[...].astype(F32)
            for degree in range(1, ORDER + 1):
                fresh = (jnp.dot(full[...], term[...], preferred_element_type=F32) * (1.0 / degree)).astype(BF16)
                running = running + fresh.astype(F32)
                if degree < ORDER:
                    term[...] = fresh
            result[i] = running.astype(BF16).reshape(2, rows, electrons)
            for copy in own_copies(i):
                copy.start()
            every[x * local + w] = result[i, o]

    begun = 0
    for i in range(mine):
        until = SKEW * last + (2 * i + 2) * PIECES
        lax.fori_loop(begun, until, chain_step, jnp.int32(0))
        begun = until
        finish(i)


    def log_copy(hop):
        other = lax.rem(x + hop, width)
        return remote(logs.at[x], logs.at[x], log_send.at[hop - 1], log_recv.at[x], {"walk": other})

    walker_id = lax.broadcasted_iota(jnp.int32, factor.shape, 0)
    weights = jnp.zeros(factor.shape, F32)
    for w in range(local):
        weights = jnp.where(walker_id == w, log_weight[w], weights)
    logs[x] = weights + factor + factor_in[0] + factor_in[1]
    for hop in range(1, width):
        log_copy(hop).start()

    def onward(w, hop_to):
        return remote(place(w), place(w), next_send.at[w], every_recv.at[x, w], {"vec": hop_to})

    def across(w, hop):
        return remote(
            place(w), place(w), across_send.at[hop - 1, w], every_recv.at[x, w], {"walk": lax.rem(x + hop, width)}
        )

    near = jnp.where(z <= last - z, 0, 1)

    def route(side, a):
        w = side * half + a
        away = jnp.where(side == 0, z, last - z)
        hop_to = jnp.where(side == 0, z + 1, z - 1)
        return w, away, last - away, hop_to

    for i in range(mine):
        for side in (near, 1 - near):
            for a in (2 * i, 2 * i + 1):
                w, away, end, hop_to = route(side, a)

                @pl.when(away > 0)
                def _():
                    onward(w, hop_to).wait_recv()

                    @pl.when(end > 0)
                    def _():
                        onward(w, hop_to).start()

                    for hop in range(1, width):
                        across(w, hop).start()

                @pl.when((away == 0) & (o != a % 2))
                def _():
                    onward(w, hop_to).wait_recv()

    for hop in range(1, width):
        other = lax.rem(x + hop, width)
        for w in range(local):
            spot = every.at[other * local + w]
            remote(spot, spot, across_send.at[hop - 1, w], every_recv.at[other, w], {"walk": other}).wait_recv()
        remote(logs.at[other], logs.at[other], log_send.at[hop - 1], log_recv.at[other], {"walk": other}).wait_recv()

    for s in range(local):
        source = copy_list[s]
        out[s] = every[source]
        out_log[s] = jnp.max(logs[source // local, pl.ds(source % local, 1), :])

    rows_copy.wait_send()
    for hop in range(1, width):
        log_copy(hop).wait_send()

    def drain(c, carry):
        for side in range(2):
            @pl.when(downstream[side] > 0)
            def _():
                chain_copy(side, c).wait_send()

        @pl.when(at_end & ((c // PIECES) % 2 != o))
        def _():
            swap_copy(c).wait_send()

        return carry

    lax.fori_loop(0, chunks, drain, jnp.int32(0))
    for side in range(2):
        @pl.when(downstream[side] > 0)
        def _():
            factor_copy(side).wait_send()

    @pl.when(at_end)
    def _():
        for i in range(mine):
            for copy in own_copies(i):
                copy.wait_send()

    for a in range(half):
        for side in range(2):
            w = side * half + a
            _, away, end, hop_to = route(side, a)

            @pl.when(away > 0)
            def _():
                @pl.when(end > 0)
                def _():
                    onward(w, hop_to).wait_send()

                for hop in range(1, width):
                    across(w, hop).wait_send()


def per_device(depth, width, walkers, inv_intersection, trial, vectors, aux_field, log_weight, copy_list):
    local, rows, electrons = walkers.shape
    count, _, orbitals = vectors.shape
    half = local // 2
    block = orbitals // 4
    span = 2 * block // count
    wide = count * span
    packed = 5 * block
    piece = packed // PIECES
    chunks = half * PIECES
    mine = half // 2
    lanes = 128
    vmem = pl.BlockSpec(memory_space=pltpu.VMEM)
    smem = pl.BlockSpec(memory_space=pltpu.SMEM)
    dma = pltpu.SemaphoreType.DMA
    out, out_log = pl.pallas_call(
        functools.partial(kernel, depth, width),
        out_shape=(
            jax.ShapeDtypeStruct(walkers.shape, BF16),
            jax.ShapeDtypeStruct((local,), F32),
        ),
        in_specs=[vmem] * 5 + [smem] * 2,
        out_specs=(vmem, smem),
        scratch_shapes=[
            pltpu.VMEM((local, rows, electrons), BF16),
            pltpu.VMEM((count, rows, electrons), BF16),
            pltpu.VMEM((local, wide), F32),
            pltpu.VMEM((local, wide), F32),
            pltpu.VMEM((local, rows, electrons), BF16),
            pltpu.VMEM((local, packed, block), F32),
            pltpu.VMEM((2, chunks, piece, block), BF16),
            pltpu.VMEM((2, chunks, piece, block), BF16),
            pltpu.VMEM((2, chunks, piece, block), BF16),
            pltpu.VMEM((orbitals, orbitals), BF16),
            pltpu.VMEM((orbitals, electrons), BF16),
            pltpu.VMEM((mine, 2, rows, electrons), BF16),
            pltpu.VMEM((width * local, rows, electrons), BF16),
            pltpu.VMEM((2, local, lanes), F32),
            pltpu.VMEM((2, local, lanes), F32),
            pltpu.VMEM((width, local, lanes), F32),
            dma((2,)),
            dma((2,)),
            dma((2, chunks)),
            dma((2, chunks)),
            dma((2,)),
            dma((2,)),
            dma((chunks,)),
            dma((chunks,)),
            dma((width, local)),
            dma((mine, 2 * width + 1)),
            dma((local,)),
            dma((max(width - 1, 1), local)),
            dma((max(width - 1, 1),)),
            dma((width,)),
        ],
        compiler_params=pltpu.CompilerParams(collective_id=0, has_side_effects=True),
    )(walkers, inv_intersection, trial, vectors, aux_field, log_weight, copy_list)
    return out, out_log


def solution(mesh):
    depth, width = mesh.shape["vec"], mesh.shape["walk"]
    assert mesh.shape["orb"] == 2 and depth > 1
    return jax.shard_map(
        functools.partial(per_device, depth, width),
        mesh=mesh,
        in_specs=(
            P(("grp", "walk"), "orb", None),
            P(("grp", "walk"), None, None),
            P(),
            P("vec", "orb", None),
            P(("grp", "walk"), "vec"),
            P(("grp", "walk")),
            P(("grp", "walk")),
        ),
        out_specs=(P(("grp", "walk"), "orb", None), P(("grp", "walk"))),
        check_vma=False,
    )
```

```python
import functools
import math

import jax
import jax.numpy as jnp
from jax import lax
from jax.experimental import pallas as pl
from jax.experimental.pallas import tpu as pltpu
from jax.sharding import PartitionSpec as P

ORDER = 6
PIECES = 4
SKEW = 4
PARTS = 2
MESH = pl.DeviceIdType.MESH
F32 = jnp.float32
BF16 = jnp.bfloat16

step_root = math.sqrt(0.08)


def remote(src, dst, send, recv, where):
    return pltpu.make_async_remote_copy(
        src_ref=src, dst_ref=dst, send_sem=send, recv_sem=recv, device_id=where, device_id_type=MESH
    )


def kernel(
    depth, width,
    walkers, inverse, trial, vectors, aux, log_weight, copy_list,
    out, out_log,
    green, mixed, bias_own, bias_in, other_rows, partial, arrived, leaving, crossed, given, operator, full, term, result, every,
    factor_in, factor_out, logs,
    bias_sems, rows_sems, chain_send, chain_recv, factor_send, factor_recv, swap_send, swap_recv, cross_recv,
    every_recv, own_sends, next_send, across_send, log_send, log_recv,
):
    z = lax.axis_index("vec")
    x = lax.axis_index("walk")
    o = lax.axis_index("orb")
    last = depth - 1
    local, rows, electrons = walkers.shape
    count, _, orbitals = vectors.shape
    half = local // 2
    block = orbitals // 4
    span = 2 * block // count
    wide = count * span
    packed = partial.shape[1]
    piece = packed // PIECES
    chunks = half * PIECES
    mine = half // 2

    barrier = pltpu.get_barrier_semaphore()

    def greet(where):
        pl.semaphore_signal(barrier, inc=1, device_id=where, device_id_type=MESH)

    greet({"orb": 1 - o})
    for hop in range(1, width):
        for core in range(2):
            greet({"walk": lax.rem(x + hop, width), "orb": core})

    @pl.when(z > 0)
    def _():
        for core in range(2):
            greet({"vec": z - 1, "orb": core})

    @pl.when(z < last)
    def _():
        for core in range(2):
            greet({"vec": z + 1, "orb": core})

    for w in range(local):
        green[w] = jnp.dot(walkers[w], inverse[w], preferred_element_type=F32).astype(BF16)
    for g in range(count):
        mixed[g] = jnp.dot(vectors[g], trial[...], preferred_element_type=F32).astype(BF16)
    gram = jnp.zeros((local * span, wide), F32)
    for j in range(rows // span):
        left = green[:, j * span:(j + 1) * span, :].reshape(local * span, electrons)
        right = mixed[:, j * span:(j + 1) * span, :].reshape(wide, electrons)
        gram = gram + lax.dot_general(left, right, (((1,), (1,)), ((), ())), preferred_element_type=F32)
    row_id = lax.broadcasted_iota(jnp.int32, (local * span, wide), 0)
    col_id = lax.broadcasted_iota(jnp.int32, (local * span, wide), 1)
    same = row_id % span == col_id % span
    folded = jnp.sum(jnp.where(same, gram, 0.0).reshape(local, span, wide), axis=1)
    wide_row = lax.broadcasted_iota(jnp.int32, (wide, wide), 0)
    wide_col = lax.broadcasted_iota(jnp.int32, (wide, wide), 1)
    groups = jnp.where(wide_row // span == wide_col // span, 1.0, 0.0).astype(F32)
    bias_own[...] = jnp.dot(folded, groups, precision=lax.Precision.HIGHEST, preferred_element_type=F32)
    pick_row = lax.broadcasted_iota(jnp.int32, (count, wide), 0)
    pick_col = lax.broadcasted_iota(jnp.int32, (count, wide), 1)
    pick = jnp.where(pick_row == pick_col // span, 1.0, 0.0).astype(F32)
    drawn = jnp.dot(aux[...], pick, precision=lax.Precision.HIGHEST, preferred_element_type=F32)
    sides = jnp.where(z > 0, 2, 0) + jnp.where(z < last, 2, 0)
    pl.semaphore_wait(barrier, 1 + 2 * (width - 1) + sides)

    rows_copy = remote(walkers, other_rows, rows_sems.at[0], rows_sems.at[1], {"orb": 1 - o})
    rows_copy.start()

    bias_copy = remote(bias_own, bias_in, bias_sems.at[0], bias_sems.at[1], {"orb": 1 - o})
    bias_copy.start()
    bias_copy.wait()
    bias = bias_own[...] + bias_in[...]
    shift = -step_root * bias
    field = drawn - shift
    factor = jnp.sum(drawn * shift - 0.5 * shift * shift, axis=1, keepdims=True) * (1.0 / span)
    factor = jnp.broadcast_to(factor, (local, logs.shape[2]))
    weighted = (field * step_root).astype(BF16).astype(F32)
    spread = jnp.broadcast_to(weighted[:, None, :], (local, span, wide)).reshape(local * span, wide)
    kron = jnp.where(same, spread, 0.0).astype(BF16)

    for j in range(block // span):
        here = slice(j * span, (j + 1) * span)
        cols = pl.ds(pl.multiple_of(o * block, block), 3 * block)
        strip = vectors[:, here, cols].reshape(wide, 3 * block)
        summed = jnp.dot(kron, strip, preferred_element_type=F32)
        for slot in range(3):
            partial[:, slot * block + j * span:slot * block + (j + 1) * span, :] = summed[
                :, slot * block:(slot + 1) * block
            ].reshape(local, span, block)
        below = slice(block + j * span, block + (j + 1) * span)
        one = vectors[:, below, pl.ds(pl.multiple_of((1 - o) * block, block), block)].reshape(wide, block)
        two = vectors[:, below, 3 * block:].reshape(wide, block)
        summed = jnp.dot(kron, jnp.concatenate([one, two], axis=1), preferred_element_type=F32)
        for slot in range(2):
            partial[:, (3 + slot) * block + j * span:(3 + slot) * block + (j + 1) * span, :] = summed[
                :, slot * block:(slot + 1) * block
            ].reshape(local, span, block)

    to_next = [z - 1, z + 1]
    upstream = [last - z, z]
    downstream = [z, last - z]

    def chain_copy(side, c):
        return remote(
            leaving.at[side, c], arrived.at[side, c], chain_send.at[side, c], chain_recv.at[side, c],
            {"vec": to_next[side]},
        )

    def factor_copy(side):
        return remote(
            factor_out.at[side], factor_in.at[side], factor_send.at[side], factor_recv.at[side],
            {"vec": to_next[side]},
        )

    def cross_copy(side, c):
        return remote(
            leaving.at[side, c], crossed.at[c], chain_send.at[side, c], cross_recv.at[c],
            {"vec": to_next[side], "orb": 1 - o},
        )

    end_side = jnp.where(z == 0, 0, 1)

    def swap_copy(c):
        return remote(leaving.at[end_side, c], given.at[c], swap_send.at[c], swap_recv.at[c], {"orb": 1 - o})

    def part_of(side, c):
        return partial[side * half + c // PIECES, pl.ds(pl.multiple_of((c % PIECES) * piece, piece), piece), :]

    def give(c, carry):
        @pl.when(((z == 0) | (z == last)) & ((c // PIECES) % 2 != o))
        def _():
            leaving[end_side, c] = part_of(end_side, c).astype(BF16)
            swap_copy(c).start()

        return carry

    lax.fori_loop(0, chunks, give, jnp.int32(0))

    def chain_step(t, carry):
        for side in range(2):
            c = t - SKEW * upstream[side]
            head = upstream[side] == 0
            owner = downstream[side] == 0

            @pl.when((c >= 0) & (c < chunks))
            def _():
                own = part_of(side, c)
                here = (c // PIECES) % 2 == o

                @pl.when(head)
                def _():
                    leaving[side, c] = own.astype(BF16)

                @pl.when(jnp.logical_not(head) & jnp.logical_not(owner))
                def _():
                    chain_copy(side, c).wait_recv()
                    leaving[side, c] = (own + arrived[side, c].astype(F32)).astype(BF16)

                @pl.when(owner & here)
                def _():
                    chain_copy(side, c).wait_recv()
                    operator[o, c] = (own + arrived[side, c].astype(F32)).astype(BF16)
                    swap_copy(c).wait_recv()
                    cross_copy(side, c).wait_recv()
                    operator[1 - o, c] = (given[c].astype(F32) + crossed[c].astype(F32)).astype(BF16)

                @pl.when(jnp.logical_not(owner) & ((downstream[side] > 1) | here))
                def _():
                    chain_copy(side, c).start()

                @pl.when((downstream[side] == 1) & jnp.logical_not(here))
                def _():
                    cross_copy(side, c).start()

                @pl.when(c == 0)
                def _():
                    @pl.when(head)
                    def _():
                        factor_in[side] = jnp.zeros_like(factor)

                    @pl.when(jnp.logical_not(head))
                    def _():
                        factor_copy(side).wait_recv()

                    @pl.when(jnp.logical_not(owner))
                    def _():
                        factor_out[side] = factor_in[side] + factor
                        factor_copy(side).start()

        return carry

    at_end = (z == 0) | (z == last)
    base = jnp.where(z == 0, 0, half)
    inward = jnp.where(z == 0, 1, last - 1)
    rows_copy.wait_recv()

    share = rows // PARTS

    def place(w, part):
        return every.at[x * local + w, pl.ds(part * share, share)]

    def own_copies(i):
        w = base + 2 * i + o
        copies = []
        for core in range(2):
            copies.append((core, {"vec": inward, "orb": core}))
        for hop in range(1, width):
            for core in range(2):
                copies.append((core, {"walk": lax.rem(x + hop, width), "orb": core}))
        copies.append((1 - o, {"orb": 1 - o}))
        return [
            remote(
                result.at[i, core, pl.ds(part * share, share)], place(w, part),
                own_sends.at[i, n, part], every_recv.at[x, w, part], where,
            )
            for part in range(PARTS)
            for n, (core, where) in enumerate(copies)
        ]

    def finish(i):
        @pl.when(at_end)
        def _():
            a = 2 * i + o
            w = base + a

            def tile(core, slot):
                flat = operator[core, pl.ds(a * PIECES, PIECES)].reshape(packed, block)
                return flat[slot * block:(slot + 1) * block, :]

            def put(r, c, value):
                full[r * block:(r + 1) * block, c * block:(c + 1) * block] = value

            spots = (((0, 0), (0, 1), (0, 2), (1, 1), (1, 3)), ((2, 1), (2, 2), (2, 3), (3, 0), (3, 3)))
            for core in range(2):
                for slot in range(5):
                    r, c = spots[core][slot]
                    value = tile(core, slot)
                    put(r, c, value)
                    if r != c:
                        put(c, r, value.T)
            term[pl.ds(pl.multiple_of(o * rows, rows), rows), :] = walkers[w]
            term[pl.ds(pl.multiple_of((1 - o) * rows, rows), rows), :] = other_rows[w]
            running = term[...].astype(F32)
            for degree in range(1, ORDER + 1):
                fresh = (jnp.dot(full[...], term[...], preferred_element_type=F32) * (1.0 / degree)).astype(BF16)
                running = running + fresh.astype(F32)
                if degree < ORDER:
                    term[...] = fresh
            result[i] = running.astype(BF16).reshape(2, rows, electrons)
            for copy in own_copies(i):
                copy.start()
            every[x * local + w] = result[i, o]

    begun = 0
    for i in range(mine):
        until = SKEW * last + (2 * i + 2) * PIECES
        lax.fori_loop(begun, until, chain_step, jnp.int32(0))
        begun = until
        finish(i)


    def log_copy(hop):
        other = lax.rem(x + hop, width)
        return remote(logs.at[x], logs.at[x], log_send.at[hop - 1], log_recv.at[x], {"walk": other})

    walker_id = lax.broadcasted_iota(jnp.int32, factor.shape, 0)
    weights = jnp.zeros(factor.shape, F32)
    for w in range(local):
        weights = jnp.where(walker_id == w, log_weight[w], weights)
    logs[x] = weights + factor + factor_in[0] + factor_in[1]
    for hop in range(1, width):
        log_copy(hop).start()

    def onward(w, part, hop_to):
        spot = place(w, part)
        return remote(spot, spot, next_send.at[w, part], every_recv.at[x, w, part], {"vec": hop_to})

    def across(w, part, hop):
        spot = place(w, part)
        return remote(
            spot, spot, across_send.at[hop - 1, w, part], every_recv.at[x, w, part], {"walk": lax.rem(x + hop, width)}
        )

    near = jnp.where(z <= last - z, 0, 1)

    def route(side, a):
        w = side * half + a
        away = jnp.where(side == 0, z, last - z)
        hop_to = jnp.where(side == 0, z + 1, z - 1)
        return w, away, last - away, hop_to

    for i in range(mine):
        for side in (near, 1 - near):
            for part, a in [(part, a) for part in range(PARTS) for a in (2 * i, 2 * i + 1)]:
                w, away, end, hop_to = route(side, a)

                @pl.when(away > 0)
                def _():
                    onward(w, part, hop_to).wait_recv()

                    @pl.when(end > 0)
                    def _():
                        onward(w, part, hop_to).start()

                    for hop in range(1, width):
                        across(w, part, hop).start()

                @pl.when((away == 0) & (o != a % 2))
                def _():
                    onward(w, part, hop_to).wait_recv()

    for hop in range(1, width):
        other = lax.rem(x + hop, width)
        for w in range(local):
            for part in range(PARTS):
                spot = every.at[other * local + w, pl.ds(part * share, share)]
                remote(
                    spot, spot, across_send.at[hop - 1, w, part], every_recv.at[other, w, part], {"walk": other}
                ).wait_recv()
        remote(logs.at[other], logs.at[other], log_send.at[hop - 1], log_recv.at[other], {"walk": other}).wait_recv()

    for s in range(local):
        source = copy_list[s]
        out[s] = every[source]
        out_log[s] = jnp.max(logs[source // local, pl.ds(source % local, 1), :])

    rows_copy.wait_send()
    for hop in range(1, width):
        log_copy(hop).wait_send()

    def drain(c, carry):
        for side in range(2):
            @pl.when(downstream[side] > 0)
            def _():
                chain_copy(side, c).wait_send()

        @pl.when(at_end & ((c // PIECES) % 2 != o))
        def _():
            swap_copy(c).wait_send()

        return carry

    lax.fori_loop(0, chunks, drain, jnp.int32(0))
    for side in range(2):
        @pl.when(downstream[side] > 0)
        def _():
            factor_copy(side).wait_send()

    @pl.when(at_end)
    def _():
        for i in range(mine):
            for copy in own_copies(i):
                copy.wait_send()

    for a in range(half):
        for side in range(2):
            w = side * half + a
            _, away, end, hop_to = route(side, a)

            @pl.when(away > 0)
            def _():
                @pl.when(end > 0)
                def _():
                    for part in range(PARTS):
                        onward(w, part, hop_to).wait_send()

                for hop in range(1, width):
                    for part in range(PARTS):
                        across(w, part, hop).wait_send()


def per_device(depth, width, walkers, inv_intersection, trial, vectors, aux_field, log_weight, copy_list):
    local, rows, electrons = walkers.shape
    count, _, orbitals = vectors.shape
    half = local // 2
    block = orbitals // 4
    span = 2 * block // count
    wide = count * span
    packed = 5 * block
    piece = packed // PIECES
    chunks = half * PIECES
    mine = half // 2
    lanes = 128
    vmem = pl.BlockSpec(memory_space=pltpu.VMEM)
    smem = pl.BlockSpec(memory_space=pltpu.SMEM)
    dma = pltpu.SemaphoreType.DMA
    out, out_log = pl.pallas_call(
        functools.partial(kernel, depth, width),
        out_shape=(
            jax.ShapeDtypeStruct(walkers.shape, BF16),
            jax.ShapeDtypeStruct((local,), F32),
        ),
        in_specs=[vmem] * 5 + [smem] * 2,
        out_specs=(vmem, smem),
        scratch_shapes=[
            pltpu.VMEM((local, rows, electrons), BF16),
            pltpu.VMEM((count, rows, electrons), BF16),
            pltpu.VMEM((local, wide), F32),
            pltpu.VMEM((local, wide), F32),
            pltpu.VMEM((local, rows, electrons), BF16),
            pltpu.VMEM((local, packed, block), F32),
            pltpu.VMEM((2, chunks, piece, block), BF16),
            pltpu.VMEM((2, chunks, piece, block), BF16),
            pltpu.VMEM((chunks, piece, block), BF16),
            pltpu.VMEM((chunks, piece, block), BF16),
            pltpu.VMEM((2, chunks, piece, block), BF16),
            pltpu.VMEM((orbitals, orbitals), BF16),
            pltpu.VMEM((orbitals, electrons), BF16),
            pltpu.VMEM((mine, 2, rows, electrons), BF16),
            pltpu.VMEM((width * local, rows, electrons), BF16),
            pltpu.VMEM((2, local, lanes), F32),
            pltpu.VMEM((2, local, lanes), F32),
            pltpu.VMEM((width, local, lanes), F32),
            dma((2,)),
            dma((2,)),
            dma((2, chunks)),
            dma((2, chunks)),
            dma((2,)),
            dma((2,)),
            dma((chunks,)),
            dma((chunks,)),
            dma((chunks,)),
            dma((width, local, PARTS)),
            dma((mine, 2 * width + 1, PARTS)),
            dma((local, PARTS)),
            dma((max(width - 1, 1), local, PARTS)),
            dma((max(width - 1, 1),)),
            dma((width,)),
        ],
        compiler_params=pltpu.CompilerParams(collective_id=0, has_side_effects=True),
    )(walkers, inv_intersection, trial, vectors, aux_field, log_weight, copy_list)
    return out, out_log


def solution(mesh):
    depth, width = mesh.shape["vec"], mesh.shape["walk"]
    assert mesh.shape["orb"] == 2 and depth > 1
    return jax.shard_map(
        functools.partial(per_device, depth, width),
        mesh=mesh,
        in_specs=(
            P(("grp", "walk"), "orb", None),
            P(("grp", "walk"), None, None),
            P(),
            P("vec", "orb", None),
            P(("grp", "walk"), "vec"),
            P(("grp", "walk")),
            P(("grp", "walk")),
        ),
        out_specs=(P(("grp", "walk"), "orb", None), P(("grp", "walk"))),
        check_vma=False,
    )
```
